32 devices in a mesh: owner: 4 (over y, core), rows: 8 (over z, x).
Axes of the slice: x: 2, y: 2, z: 4, core: 2. Of those that a mesh axis runs over, the one named last changes fastest.
Arguments:
- w_gate: float32 [64, 2048, 1024], P('owner', 'rows'), may hold values from -0.1875 to 0.1875
- avg_gate: float32 [64, 2048, 1024], P('owner', 'rows'), may hold values from -0.125 to 0.125
- w_up: float32 [64, 2048, 1024], P('owner', 'rows'), may hold values from -0.1875 to 0.1875
- avg_up: float32 [64, 2048, 1024], P('owner', 'rows'), may hold values from -0.125 to 0.125
- mix_share: float32 [64], P('owner'), may hold values from 0.2 to 0.8
- router_weight: float32 [2048, 64], P('rows', 'owner'), may hold values from -0.125 to 0.125
- router_gain: float32 [2048], P('rows'), may hold values from 0.25 to 1.75
Outputs:
- serve_gate: bfloat16 [64, 2048, 1024], P('owner', None, 'rows')
- serve_up: bfloat16 [64, 2048, 1024], P('owner', None, 'rows')
- scale_gate: float32 [64, 1024], P('owner', 'rows')
- scale_up: float32 [64, 1024], P('owner', 'rows')
- serve_router: bfloat16 [2048, 64], replicated
The draws below stay inside these ranges and needn't reach their ends.
All inputs are finite; a program needn't handle non-finite values.
Results may differ from the reference program's by a relative error of at most 0.001.
Values may be sent and summed in bfloat16 or wider, within the bound.
No kernel may reach another device: no remote copies, remote signals or barrier semaphores. Data moves between devices by JAX's collectives and lax.ppermute only.
A program may use at most 256 MiB of HBM per device.

```python
import jax
import jax.numpy as jnp
from jax import lax

EXPERTS = 64
D_MODEL = 2048
D_EXPERT = 1024


def raised(array, key, source, target, parts, factor):
    owner, partner = [(jnp.arange(array.shape[position]) // (array.shape[position] // parts)).reshape([-1 if axis == position else 1 for axis in range(array.ndim)]) for position in (source, target)]
    chosen = jax.random.permutation(key, parts)[partner]
    strong = (owner == chosen) | (owner == (partner + parts // 2) % parts)
    return jnp.where(strong, factor * array, array)


def levels(key, dims, split, smallest, high):
    def one(dim, blocks):
        steps = jax.random.uniform(jax.random.fold_in(jax.random.fold_in(key, 6), dim), (blocks,), jnp.float32, smallest / len(split), high / len(split))
        return jnp.repeat(jnp.exp(steps), dims[dim] // blocks).reshape((-1,) + (1,) * (len(dims) - dim - 1))

    level = one(*split[0])
    for cut in split[1:]:
        level = level * one(*cut)
    return level


def scatter_about(rng, extent, deviation, most, split=(), kind=jnp.bfloat16):
    gain = levels(rng, extent, split, -0.22, 0.18) if split else 1.0
    result = jax.random.normal(rng, extent, jnp.float32) * deviation * gain
    return jnp.minimum(jnp.maximum(result, -most), most).astype(kind)


def noise_with(stream_key, dims, spread, reach, shards, heavy, dtype=jnp.bfloat16):
    entries = spread * jax.random.normal(stream_key, dims, jnp.float32)
    if shards:
        entries = entries * levels(stream_key, dims, shards, -0.22, 0.18)
    return jnp.clip(raised(entries, jax.random.fold_in(stream_key, 3), *heavy), -reach, reach).astype(dtype)


def setup_inputs(seed: int = 0) -> dict:
    seeds = jax.random.split(jax.random.key(seed), 8)
    w_gate = noise_with(seeds[0], (EXPERTS, D_MODEL, D_EXPERT), D_MODEL ** -0.5, 0.1875, ((0, 4), (1, 8)), (1, 2, 8, 2.0), jnp.float32)
    avg_gate = scatter_about(seeds[1], (EXPERTS, D_MODEL, D_EXPERT), D_MODEL ** -0.5, 0.125, ((0, 4), (1, 8)), jnp.float32)
    w_up = noise_with(seeds[2], (EXPERTS, D_MODEL, D_EXPERT), D_MODEL ** -0.5, 0.1875, ((0, 4), (1, 8)), (1, 2, 8, 2.0), jnp.float32)
    avg_up = scatter_about(seeds[3], (EXPERTS, D_MODEL, D_EXPERT), D_MODEL ** -0.5, 0.125, ((0, 4), (1, 8)), jnp.float32)
    mix_share = jnp.clip(0.2 + 0.6 * jax.random.uniform(seeds[4], (EXPERTS,), jnp.float32) ** levels(seeds[4], (EXPERTS,), ((0, 4),), -0.2, 0.2), 0.2, 0.8)
    router_weight = scatter_about(seeds[5], (D_MODEL, EXPERTS), D_MODEL ** -0.5, 0.125, ((0, 8), (1, 4)), jnp.float32)
    router_gain = jnp.clip(1.0 + 0.15 * jax.random.normal(seeds[6], (D_MODEL,), jnp.float32), 0.25, 1.75)
    return dict(w_gate=w_gate, avg_gate=avg_gate, w_up=w_up, avg_up=avg_up, mix_share=mix_share, router_weight=router_weight, router_gain=router_gain)


def reference(w_gate, avg_gate, w_up, avg_up, mix_share, router_weight, router_gain):
    fresh_gate = mix_share[:, None, None] * w_gate + (1.0 - mix_share[:, None, None]) * avg_gate
    fresh_up = mix_share[:, None, None] * w_up + (1.0 - mix_share[:, None, None]) * avg_up
    scale_gate = jnp.sqrt(lax.optimization_barrier(jnp.sum(fresh_gate * fresh_gate, axis=1)))
    serve_gate = (fresh_gate / jnp.expand_dims(scale_gate, 1)).astype(jnp.bfloat16)
    scale_up = jnp.sqrt(lax.optimization_barrier(jnp.sum(fresh_up * fresh_up, axis=1)))
    serve_up = (fresh_up / jnp.expand_dims(scale_up, 1)).astype(jnp.bfloat16)
    serve_router = (router_weight * router_gain[:, None]).astype(jnp.bfloat16)
    return (serve_gate, serve_up, scale_gate, scale_up, serve_router)
```

```python
import jax
import jax.numpy as jnp
from jax import lax
from jax.experimental import pallas as pl
from jax.experimental.pallas import tpu as pltpu
from jax.sharding import PartitionSpec as P

F32 = jnp.float32
BF16 = jnp.bfloat16


def params():
    return pltpu.CompilerParams(dimension_semantics=("arbitrary",), vmem_limit_bytes=48 * 2**20)


def mixed(share_ref, expert, w, avg):
    share = share_ref[expert]
    return share * w + (1.0 - share) * avg


def sums_kernel(share_ref, wg_ref, ag_ref, wu_ref, au_ref, gate_ref, up_ref):
    expert = pl.program_id(0)
    for w_ref, avg_ref, out_ref in ((wg_ref, ag_ref, gate_ref), (wu_ref, au_ref, up_ref)):
        fresh = mixed(share_ref, expert, w_ref[0], avg_ref[0])
        out_ref[0] = jnp.sum(fresh * fresh, axis=0, keepdims=True)


def sums(share, *arrays):
    experts, rows, width = arrays[0].shape
    block = pl.BlockSpec((1, rows, width), lambda e: (e, 0, 0))
    total = pl.BlockSpec((1, 1, width), lambda e: (e, 0, 0))
    return pl.pallas_call(
        sums_kernel,
        grid=(experts,),
        in_specs=[pl.BlockSpec(memory_space=pltpu.SMEM)] + [block] * 4,
        out_specs=[total] * 2,
        out_shape=[jax.ShapeDtypeStruct((experts, 1, width), F32)] * 2,
        compiler_params=params(),
        cost_estimate=pl.CostEstimate(
            flops=10 * experts * rows * width, bytes_accessed=16 * experts * rows * width, transcendentals=0
        ),
        name="sums",
    )(share, *arrays)


def narrow_kernel(share_ref, w_ref, avg_ref, inverse_ref, out_ref):
    expert = pl.program_id(0)
    parts, _, _, columns = out_ref.shape
    for part in range(parts):
        cut = slice(part * columns, (part + 1) * columns)
        fresh = mixed(share_ref, expert, w_ref[0, :, cut], avg_ref[0, :, cut])
        out_ref[part, 0] = (fresh * inverse_ref[0, :, cut]).astype(BF16)


def narrow(share, w, avg, inverse, parts):
    experts, rows, width = w.shape
    columns = width // parts
    block = pl.BlockSpec((1, rows, width), lambda e: (e, 0, 0))
    return pl.pallas_call(
        narrow_kernel,
        grid=(experts,),
        in_specs=[
            pl.BlockSpec(memory_space=pltpu.SMEM),
            block,
            block,
            pl.BlockSpec((1, 1, width), lambda e: (e, 0, 0)),
        ],
        out_specs=pl.BlockSpec((parts, 1, rows, columns), lambda e: (0, e, 0, 0)),
        out_shape=jax.ShapeDtypeStruct((parts, experts, rows, columns), BF16),
        compiler_params=params(),
        cost_estimate=pl.CostEstimate(
            flops=5 * experts * rows * width, bytes_accessed=10 * experts * rows * width, transcendentals=0
        ),
        name="narrow",
    )(share, w, avg, inverse)


def unpack_kernel(in_ref, out_ref):
    parts, _, rows, _ = in_ref.shape
    for part in range(parts):
        out_ref[0, part * rows : (part + 1) * rows] = in_ref[part, 0]


def unpack(arrived):
    parts, experts, rows, columns = arrived.shape
    return pl.pallas_call(
        unpack_kernel,
        grid=(experts,),
        in_specs=[pl.BlockSpec((parts, 1, rows, columns), lambda e: (0, e, 0, 0))],
        out_specs=pl.BlockSpec((1, parts * rows, columns), lambda e: (e, 0, 0)),
        out_shape=jax.ShapeDtypeStruct((experts, parts * rows, columns), BF16),
        compiler_params=params(),
        cost_estimate=pl.CostEstimate(
            flops=arrived.size, bytes_accessed=4 * arrived.size, transcendentals=0
        ),
        name="unpack",
    )(arrived)


def body(parts, w_gate, avg_gate, w_up, avg_up, mix_share, router_weight, router_gain):
    experts, _, width = w_gate.shape
    columns = width // parts

    part_router = (router_weight * router_gain[:, None]).astype(BF16)
    gathered = lax.all_gather(part_router, ("rows", "owner"), axis=0)
    owners = gathered.shape[0] // parts
    router_rows, router_columns = part_router.shape

    partial_gate, partial_up = sums(mix_share, w_gate, avg_gate, w_up, avg_up)
    partial = jnp.concatenate([partial_gate, partial_up]).reshape(2 * experts, parts, columns)
    pieces = lax.all_to_all(partial.transpose(1, 0, 2), "rows", split_axis=0, concat_axis=0, tiled=True)
    scale = jnp.sqrt(jnp.sum(pieces, axis=0))
    scale_gate, scale_up = scale[:experts], scale[experts:]
    inverse = lax.all_gather(1.0 / scale, "rows", axis=0)
    inverse = inverse.transpose(1, 0, 2).reshape(2, experts, 1, width)
    inverse, gathered = lax.optimization_barrier((inverse, gathered))
    serve_router = (
        gathered.reshape(parts, owners, router_rows, router_columns)
        .transpose(0, 2, 1, 3)
        .reshape(parts * router_rows, owners * router_columns)
    )

    def exchange(packed):
        return lax.all_to_all(packed, "rows", split_axis=0, concat_axis=0, tiled=True)

    packed_gate = narrow(mix_share, w_gate, avg_gate, inverse[0], parts)
    arrived_gate = exchange(packed_gate)
    packed_up = narrow(mix_share, w_up, avg_up, inverse[1], parts)
    arrived_up = exchange(packed_up)
    return (unpack(arrived_gate), unpack(arrived_up), scale_gate, scale_up, serve_router)


def solution(mesh):
    parts = mesh.shape["rows"]
    matrix = P("owner", "rows", None)
    in_specs = (matrix, matrix, matrix, matrix, P("owner"), P("rows", "owner"), P("rows"))
    served = P("owner", None, "rows")
    out_specs = (served, served, P("owner", "rows"), P("owner", "rows"), P())

    def step(*arguments):
        return body(parts, *arguments)

    return jax.shard_map(step, mesh=mesh, in_specs=in_specs, out_specs=out_specs, check_vma=False)
```

```python
import functools

import jax
import jax.numpy as jnp
from jax import lax
from jax.experimental import pallas as pl
from jax.experimental.pallas import tpu as pltpu
from jax.sharding import PartitionSpec as P

F32 = jnp.float32
BF16 = jnp.bfloat16


def params():
    return pltpu.CompilerParams(dimension_semantics=("arbitrary",), vmem_limit_bytes=48 * 2**20)


def mixed(share_ref, expert, w, avg):
    share = share_ref[expert]
    return share * w + (1.0 - share) * avg


def sums_kernel(share_ref, wg_ref, ag_ref, wu_ref, au_ref, gate_ref, up_ref):
    expert = pl.program_id(0)
    for w_ref, avg_ref, out_ref in ((wg_ref, ag_ref, gate_ref), (wu_ref, au_ref, up_ref)):
        fresh = mixed(share_ref, expert, w_ref[0], avg_ref[0])
        out_ref[0] = jnp.sum(fresh * fresh, axis=0, keepdims=True)


def sums(share, *arrays):
    experts, rows, width = arrays[0].shape
    block = pl.BlockSpec((1, rows, width), lambda e: (e, 0, 0))
    total = pl.BlockSpec((1, 1, width), lambda e: (e, 0, 0))
    return pl.pallas_call(
        sums_kernel,
        grid=(experts,),
        in_specs=[pl.BlockSpec(memory_space=pltpu.SMEM)] + [block] * 4,
        out_specs=[total] * 2,
        out_shape=[jax.ShapeDtypeStruct((experts, 1, width), F32)] * 2,
        compiler_params=params(),
        cost_estimate=pl.CostEstimate(
            flops=10 * experts * rows * width, bytes_accessed=16 * experts * rows * width, transcendentals=0
        ),
        name="sums",
    )(share, *arrays)


def narrow_kernel(first, share_ref, w_ref, avg_ref, inverse_ref, *refs):
    out_ref = refs[-1]
    expert = first + pl.program_id(0)
    parts, _, _, columns = out_ref.shape
    for part in range(parts):
        cut = slice(part * columns, (part + 1) * columns)
        fresh = mixed(share_ref, expert, w_ref[0, :, cut], avg_ref[0, :, cut])
        out_ref[part, 0] = (fresh * inverse_ref[0, :, cut]).astype(BF16)


def narrow(share, w, avg, inverse, parts, first, count, total, at=0, buffer=()):
    _, rows, width = w.shape
    columns = width // parts
    block = pl.BlockSpec((1, rows, width), lambda e: (first + e, 0, 0))
    return pl.pallas_call(
        functools.partial(narrow_kernel, first),
        grid=(count,),
        in_specs=[
            pl.BlockSpec(memory_space=pltpu.SMEM),
            block,
            block,
            pl.BlockSpec((1, 1, width), lambda e: (first + e, 0, 0)),
        ]
        + [pl.BlockSpec(memory_space=pl.ANY)] * len(buffer),
        out_specs=pl.BlockSpec((parts, 1, rows, columns), lambda e: (0, at + e, 0, 0)),
        out_shape=jax.ShapeDtypeStruct((parts, total, rows, columns), BF16),
        input_output_aliases={4: 0} if buffer else {},
        compiler_params=params(),
        cost_estimate=pl.CostEstimate(
            flops=5 * count * rows * width, bytes_accessed=10 * count * rows * width, transcendentals=0
        ),
        name="narrow",
    )(share, w, avg, inverse, *buffer)


def unpack_kernel(in_ref, *refs):
    out_ref = refs[-1]
    parts, _, rows, _ = in_ref.shape
    for part in range(parts):
        out_ref[0, part * rows : (part + 1) * rows] = in_ref[part, 0]


def unpack(arrived, first, count, total, at=0, buffer=()):
    parts, _, rows, columns = arrived.shape
    moved = parts * count * rows * columns
    return pl.pallas_call(
        unpack_kernel,
        grid=(count,),
        in_specs=[pl.BlockSpec((parts, 1, rows, columns), lambda e: (0, first + e, 0, 0))]
        + [pl.BlockSpec(memory_space=pl.ANY)] * len(buffer),
        out_specs=pl.BlockSpec((1, parts * rows, columns), lambda e: (at + e, 0, 0)),
        out_shape=jax.ShapeDtypeStruct((total, parts * rows, columns), BF16),
        input_output_aliases={1: 0} if buffer else {},
        compiler_params=params(),
        cost_estimate=pl.CostEstimate(flops=moved, bytes_accessed=4 * moved, transcendentals=0),
        name="unpack",
    )(arrived, *buffer)


def exchange(packed, axes="rows"):
    return lax.all_to_all(packed, axes, split_axis=0, concat_axis=0, tiled=True)


def to_all(block, axes, members):
    return exchange(jnp.broadcast_to(block, (members,) + block.shape), axes)


def body(parts, owners, w_gate, avg_gate, w_up, avg_up, mix_share, router_weight, router_gain):
    experts, _, width = w_gate.shape

    part_router = (router_weight * router_gain[:, None]).astype(BF16).T
    gathered = to_all(part_router, ("rows", "owner"), parts * owners)

    partial_gate, partial_up = sums(mix_share, w_gate, avg_gate, w_up, avg_up)
    partial = jnp.concatenate([partial_gate, partial_up]).reshape(2 * experts, parts, width // parts)
    pieces = exchange(partial.transpose(1, 0, 2))
    scale = jnp.sqrt(jnp.sum(pieces, axis=0))
    scale_gate, scale_up = scale[:experts], scale[experts:]
    inverse = to_all(1.0 / scale, "rows", parts)
    inverse = inverse.transpose(1, 0, 2).reshape(2, experts, 1, width)
    inverse, gathered = lax.optimization_barrier((inverse, gathered))
    router_columns, router_rows = part_router.shape
    serve_router = (
        gathered.reshape(parts, owners, router_columns, router_rows)
        .transpose(1, 2, 0, 3)
        .reshape(owners * router_columns, parts * router_rows)
        .T
    )

    few = max(1, experts // 4)
    rest = experts - few
    packed_first = narrow(mix_share, w_gate, avg_gate, inverse[0], parts, 0, few, few)
    arrived_first = exchange(packed_first)
    packed = narrow(mix_share, w_gate, avg_gate, inverse[0], parts, few, rest, 2 * rest)
    packed = narrow(mix_share, w_up, avg_up, inverse[1], parts, 0, rest, 2 * rest, rest, (packed,))
    arrived = exchange(packed)
    packed_last = narrow(mix_share, w_up, avg_up, inverse[1], parts, rest, few, few)
    arrived_last = exchange(packed_last)

    serve_gate = unpack(arrived_first, 0, few, experts)
    serve_gate = unpack(arrived, 0, rest, experts, few, (serve_gate,))
    serve_up = unpack(arrived, rest, rest, experts)
    serve_up = unpack(arrived_last, 0, few, experts, rest, (serve_up,))
    return (serve_gate, serve_up, scale_gate, scale_up, serve_router)


def solution(mesh):
    parts, owners = mesh.shape["rows"], mesh.shape["owner"]
    matrix = P("owner", "rows", None)
    in_specs = (matrix, matrix, matrix, matrix, P("owner"), P("rows", "owner"), P("rows"))
    served = P("owner", None, "rows")
    out_specs = (served, served, P("owner", "rows"), P("owner", "rows"), P())

    def step(*arguments):
        return body(parts, owners, *arguments)

    return jax.shard_map(step, mesh=mesh, in_specs=in_specs, out_specs=out_specs, check_vma=False)
```
